32 devices in a mesh: lon: 4 (over z), lat: 4 (over x, core), mem: 2 (over y).
Axes of the slice: x: 2, y: 2, z: 4, core: 2. Of those that a mesh axis runs over, the one named last changes fastest.
Arguments:
- tokens: bfloat16 [4, 8, 136, 24, 192], P('mem', None, 'lat', 'lon'), parts along dimension 0, may hold values from -6 to 6
- band_rows: int32 [4, 2], P('lat'), may hold values from 0 to 89, as said below
- down_gain: float32 [768], replicated, may hold values from 0.1 to 1.9
- down_shift: float32 [768], replicated, may hold values from -3 to 3
- down_weight: bfloat16 [768, 384], P(('lon', 'lat')), may hold values from -0.21875 to 0.21875
- up_weight: bfloat16 [384, 768], P(('lon', 'lat')), may hold values from -0.3125 to 0.3125
- up_gain: float32 [192], replicated, may hold values from 0.1 to 1.9
- up_shift: float32 [192], replicated, may hold values from -3 to 3
- mix_weight: bfloat16 [192, 192], replicated, may hold values from -0.4375 to 0.4375
Outputs:
- expanded: bfloat16 [4, 8, 136, 24, 192], P('mem', None, 'lat', 'lon'), parts along dimension 0
The draws below stay inside these ranges and needn't reach their ends.
There are 2 independent parts, one for each index of `mem`. The reference program is written for one: setup_inputs(seed, part) draws one part's arguments, and reference() takes and returns one part's arrays. A program takes and returns all parts, laid end to end along the dimension named above; an argument that names none is the same for every part. Nothing has to cross between parts.
Inputs may be any that keep to these rules, and one draw needn't show every extreme that they name: `band_rows`: row b holds band b's first latitude row and one past its last; the bands cover rows 0 to 88 in order without gaps; band 0 holds an odd number of rows and every other band an even number; each band holds at least 2 * (5) rows and at most 34, and some band other than band 0 holds exactly 34.
All inputs are finite; a program needn't handle non-finite values.
Results may differ from the reference program's by a relative error of at most 0.0062.
Values may be sent and summed in bfloat16 or wider, within the bound.
A program may use at most 64 MiB of HBM per device.

```python
import jax
import jax.numpy as jnp
from jax import lax

C = 192
LEVELS = 8
MEMBERS = 2
BAND_ROWS = 22
BAND_ROW_SLOTS = 34
SLOTS = 136
LAT = 89
LON = 24
N_LAT = 4


def draw_band_rows(key, part):
    bands = N_LAT
    half_least = BAND_ROWS // 4
    slot_half = BAND_ROW_SLOTS // 2
    band_ids = jnp.arange(bands, dtype=jnp.int32)
    fullest = jax.random.randint(jax.random.fold_in(key, 11), (), 1, bands, dtype=jnp.int32)
    weights = jax.random.randint(jax.random.fold_in(key, 12), (bands,), 500, 1001, dtype=jnp.int32)
    order_keys = jax.random.permutation(jax.random.fold_in(key, 13), bands).astype(jnp.int32)
    sharing = band_ids != fullest
    weights = jnp.where(sharing, weights, 0)
    spare_halves = BAND_ROWS * bands // 2 - slot_half - (bands - 1) * half_least
    half_shares = spare_halves * weights // jnp.sum(weights)
    leftover = spare_halves - jnp.sum(half_shares)
    earlier = sharing[None, :] & (order_keys[None, :] < order_keys[:, None])
    ranking = jnp.sum(earlier.astype(jnp.int32), axis=1)
    extra_halves = (sharing & (ranking < leftover)).astype(jnp.int32)
    halves = jnp.where(band_ids == fullest, slot_half, half_least + half_shares + extra_halves)
    row_counts = (2 * halves + (band_ids == 0).astype(jnp.int32)).astype(jnp.int32)
    starts = jnp.cumsum(row_counts) - row_counts
    return jnp.stack([starts, starts + row_counts], axis=1).astype(jnp.int32)


def level_of(stream_key, extent, shards, smallest, top_value):
    def one(axis_at, parts):
        heights = jax.random.uniform(jax.random.fold_in(jax.random.fold_in(stream_key, 6), axis_at), (parts,), jnp.float32, smallest / len(shards), top_value / len(shards))
        return jnp.repeat(jnp.exp(heights), extent[axis_at] // parts).reshape((-1,) + (1,) * (len(extent) - axis_at - 1))

    level = one(*shards[0])
    for cut in shards[1:]:
        level = level * one(*cut)
    return level


def scatter_about(rng, dims, scale, most, cuts=(), kind=jnp.bfloat16):
    values = scale * jax.random.normal(rng, dims, jnp.float32)
    if cuts:
        values = values * level_of(rng, dims, cuts, -0.22, 0.18)
    return jnp.clip(values, -most, most).astype(kind)


def setup_inputs(seed: int = 0, part: int = 0) -> dict:
    streams_of = jax.random.split(jax.random.key(seed), 10)
    part_keys = jax.random.split(jax.random.fold_in(streams_of[9], part), 10)
    return {
        "tokens": scatter_about(part_keys[0], (MEMBERS, LEVELS, SLOTS, LON, C), 1.0, 6.0, ((2, 4), (3, 4))),
        "band_rows": draw_band_rows(jax.random.fold_in(streams_of[9], 71), part),
        "down_gain": jnp.clip(1.0 + 0.18 * jax.random.normal(streams_of[2], (4 * C,), jnp.float32), 0.1, 1.9),
        "down_shift": scatter_about(streams_of[3], (4 * C,), 0.5, 3.0, (), jnp.float32),
        "down_weight": scatter_about(streams_of[4], (4 * C, 2 * C), (4 * C) ** -0.5, 0.21875, ((0, 16),)),
        "up_weight": scatter_about(streams_of[5], (2 * C, 4 * C), (2 * C) ** -0.5, 0.3125, ((0, 16),)),
        "up_gain": jnp.clip(1.0 + 0.18 * jax.random.normal(streams_of[6], (C,), jnp.float32), 0.1, 1.9),
        "up_shift": scatter_about(streams_of[7], (C,), 0.5, 3.0, (), jnp.float32),
        "mix_weight": scatter_about(streams_of[8], (C, C), C ** -0.5, 0.4375),
    }


def normalize(values, scale_gain, bias_shift):
    average = lax.optimization_barrier(jnp.mean(values, axis=-1, keepdims=True))
    centred = values - average
    spread = lax.optimization_barrier(jnp.mean(centred * centred, axis=-1, keepdims=True))
    return centred * lax.rsqrt(spread + 1e-05) * scale_gain + bias_shift

def reference(tokens, band_rows, down_gain, down_shift, down_weight, up_weight, up_gain, up_shift, mix_weight):
    band_starts = band_rows[:, 0].astype(jnp.int32)
    band_ends = band_rows[:, 1].astype(jnp.int32)
    lat_rows = jnp.arange(LAT, dtype=jnp.int32)
    band_of = (lax.optimization_barrier(jnp.sum((lat_rows[:, None] >= band_starts[None, :]).astype(jnp.int32), axis=1)) - 1).astype(jnp.int32)
    source = (band_of * BAND_ROW_SLOTS + lat_rows - jnp.take(band_starts, band_of)).astype(jnp.int32)
    half_lat = (LAT + 1) // 2
    half_lon = LON // 2
    slot_ids = jnp.arange(SLOTS, dtype=jnp.int32)
    slot_band = (slot_ids // BAND_ROW_SLOTS).astype(jnp.int32)
    local_row = (slot_ids % BAND_ROW_SLOTS).astype(jnp.int32)
    live_rows = jnp.take(band_ends, slot_band) - jnp.take(band_starts, slot_band)
    global_row = (jnp.take(band_starts, slot_band) + local_row).astype(jnp.int32)
    is_live = local_row < live_rows
    safe_row = jnp.minimum(global_row, LAT - 1).astype(jnp.int32)

    def one_level(level_plane):
        field = jnp.take(level_plane, source, axis=0)
        field = jnp.pad(field, ((0, 1), (0, 0), (0, 0)))
        field = jnp.roll(field, -1, axis=1)
        blocks = field.reshape(half_lat, 2, half_lon, 2, C).transpose(0, 2, 3, 1, 4).reshape(half_lat * half_lon, 4 * C)
        merged_norm = normalize(blocks.astype(jnp.float32), down_gain, down_shift).astype(jnp.bfloat16)
        coarse = jnp.dot(merged_norm, down_weight, preferred_element_type=jnp.float32).astype(jnp.bfloat16)
        grown = jnp.dot(coarse, up_weight, preferred_element_type=jnp.float32)
        grown = grown.reshape(half_lat, half_lon, 2, 2, C).transpose(0, 2, 1, 3, 4).reshape(2 * half_lat, 2 * half_lon, C)[:LAT]
        grown = jnp.roll(grown, 1, axis=1)
        fine_norm = normalize(grown, up_gain, up_shift).astype(jnp.bfloat16)
        fine_out = jnp.dot(fine_norm.reshape(LAT * LON, C), mix_weight, preferred_element_type=jnp.float32)
        fine_out = fine_out.astype(jnp.bfloat16).reshape(LAT, LON, C)
        picked = jnp.take(fine_out, safe_row, axis=0)
        return jnp.where(is_live[:, None, None], picked, jnp.zeros_like(picked))
    planes = tokens.reshape(MEMBERS * LEVELS, SLOTS, LON, C)
    results = lax.map(one_level, planes)
    return results.reshape(MEMBERS, LEVELS, SLOTS, LON, C)
```

```python
import functools

import jax
import jax.numpy as jnp
from jax import lax
from jax.experimental import pallas as pl
from jax.experimental.pallas import tpu as pltpu
from jax.sharding import PartitionSpec as P

LANES = 128
SUBLANES = 8


def shifted(block, axis, distance):
    devices = range(lax.axis_size(axis))
    route = [((i - distance) % len(devices), i) for i in devices]
    return lax.ppermute(block, axis, route)


def passed_along(block, axis, distance):
    devices = range(lax.axis_size(axis))
    route = [(i - distance, i) for i in devices if i - distance in devices]
    return lax.ppermute(block, axis, route)


def normalized(planes, gains, shifts, width):
    total = functools.reduce(jnp.add, planes)
    average = jnp.sum(total, axis=-1, keepdims=True) * (1.0 / width)
    centred = [plane - average for plane in planes]
    squares = functools.reduce(jnp.add, [c * c for c in centred])
    spread = jnp.sum(squares, axis=-1, keepdims=True) * (1.0 / width)
    scale = lax.rsqrt(spread + 1e-05)
    return [
        (c * scale * gain + shift).astype(jnp.bfloat16)
        for c, gain, shift in zip(centred, gains, shifts)
    ]


def compute_kernel(
    band_ref, tokens_ref, west_ref, east_ref, north_ref, south_ref,
    down_gain_ref, down_shift_ref, down_weight_ref, up_weight_ref,
    up_gain_ref, up_shift_ref, mix_ref, out_ref, low_ref, high_ref, side_low, side_high,
):
    units, slots, columns, features = tokens_ref.shape
    pitch = -(-(columns + 2) // SUBLANES) * SUBLANES
    half_pitch = pitch // 2
    half_rows = slots // 2 + 1
    plane_rows = low_ref.shape[1] // 2
    patches = half_rows * half_pitch
    rest = features - LANES
    first_row = band_ref[0, 0]
    live = band_ref[0, 1] - first_row
    odd = lax.rem(first_row, 2)

    def cell(row):
        moved = row + odd
        at = lax.rem(moved, 2) * plane_rows + SUBLANES + pitch * (moved // 2)
        return pl.multiple_of(at, SUBLANES)

    def put(unit, at, count, values):
        low_ref[unit, pl.ds(at, count), :] = values[:, :LANES]
        high_ref[unit, pl.ds(at, count), :rest] = values[:, LANES:]

    def fill(unit, carry):
        for row in range(slots):
            put(unit, cell(row), columns, tokens_ref[unit, row].astype(jnp.float32))
        for side_ref, offset in ((west_ref, -1), (east_ref, columns)):
            side = side_ref[unit].astype(jnp.float32)
            side_low[...] = side[:, :LANES]
            side_high[:, :rest] = side[:, LANES:]
            for parity in range(2):
                at = cell(parity) + offset
                reads = pl.ds(parity, slots // 2, stride=2)
                writes = pl.ds(at, slots // 2, stride=pitch)
                low_ref[unit, writes, :] = side_low[reads, :]
                high_ref[unit, writes, :] = side_high[reads, :]

        def whole_row(values, row):
            at = cell(row)
            put(unit, at, columns + 1, values[: columns + 1])
            put(unit, at - 1, 1, values[columns + 1 : columns + 2])

        @pl.when(odd == 1)
        def _():
            whole_row(north_ref[unit].astype(jnp.float32), -1)

        whole_row(south_ref[unit].astype(jnp.float32), live)
        return carry

    lax.fori_loop(0, units, fill, 0)

    def plane(p, q):
        reads = pl.ds(p * plane_rows + SUBLANES - 1 + q, patches, stride=2)
        lows = [low_ref[unit, reads, :] for unit in range(units)]
        highs = [high_ref[unit, reads, :][:, :rest] for unit in range(units)]
        return jnp.concatenate([jnp.concatenate(lows, 0), jnp.concatenate(highs, 0)], 1)

    order = [(p, q) for q in range(2) for p in range(2)]
    gains = [down_gain_ref[i : i + 1] for i in range(4)]
    shifts = [down_shift_ref[i : i + 1] for i in range(4)]
    merged = normalized([plane(p, q) for p, q in order], gains, shifts, 4 * features)
    coarse = functools.reduce(
        jnp.add,
        [
            jnp.dot(
                part,
                down_weight_ref[i * features : (i + 1) * features],
                preferred_element_type=jnp.float32,
            )
            for i, part in enumerate(merged)
        ],
    ).astype(jnp.bfloat16)
    for i, (p, q) in enumerate((p, q) for p in range(2) for q in range(2)):
        grown = jnp.dot(
            coarse,
            up_weight_ref[:, i * features : (i + 1) * features],
            preferred_element_type=jnp.float32,
        )
        (fine,) = normalized([grown], [up_gain_ref[...]], [up_shift_ref[...]], features)
        fine_out = jnp.dot(fine, mix_ref[...], preferred_element_type=jnp.float32)
        writes = pl.ds(p * plane_rows + SUBLANES - 1 + q, patches, stride=2)
        for unit in range(units):
            piece = fine_out[unit * patches : (unit + 1) * patches]
            low_ref[unit, writes, :] = piece[:, :LANES]
            high_ref[unit, writes, :] = jnp.concatenate(
                [piece[:, LANES:], piece[:, LANES:]], 1
            ) if rest * 2 == LANES else jnp.pad(piece[:, LANES:], ((0, 0), (0, LANES - rest)))

    def drain(unit, carry):
        for row in range(slots):
            at = cell(row)
            values = jnp.concatenate(
                [low_ref[unit, pl.ds(at, columns), :], high_ref[unit, pl.ds(at, columns), :rest]], 1
            )
            values = jnp.where(row < live, values, jnp.zeros_like(values))
            out_ref[unit, row] = values.astype(jnp.bfloat16)
        return carry

    lax.fori_loop(0, units, drain, 0)


def compute(tokens, band_rows, sides, norms, weights, block=4):
    units, slots, columns, features = tokens.shape
    pitch = -(-(columns + 2) // SUBLANES) * SUBLANES
    plane_rows = SUBLANES + pitch * (slots // 2 + 1)
    down_gain, down_shift, up_gain, up_shift = norms

    def per_unit(*shape):
        return pl.BlockSpec((block, *shape), lambda i: (i,) + (0,) * len(shape))

    def whole(array):
        return pl.BlockSpec(array.shape, lambda i: (0,) * array.ndim)

    params = [
        down_gain.reshape(4, features), down_shift.reshape(4, features), weights[0], weights[1],
        up_gain.reshape(1, features), up_shift.reshape(1, features), weights[2],
    ]
    return pl.pallas_call(
        compute_kernel,
        grid=(units // block,),
        out_shape=jax.ShapeDtypeStruct(tokens.shape, tokens.dtype),
        in_specs=[
            pl.BlockSpec(memory_space=pltpu.SMEM),
            per_unit(slots, columns, features),
            per_unit(slots, features),
            per_unit(slots, features),
            per_unit(columns + 2, features),
            per_unit(columns + 2, features),
            *[whole(p) for p in params],
        ],
        out_specs=per_unit(slots, columns, features),
        scratch_shapes=[
            pltpu.VMEM((block, 2 * plane_rows, LANES), jnp.float32),
            pltpu.VMEM((block, 2 * plane_rows, LANES), jnp.float32),
            pltpu.VMEM((slots, LANES), jnp.float32),
            pltpu.VMEM((slots, LANES), jnp.float32),
        ],
        compiler_params=pltpu.CompilerParams(dimension_semantics=("arbitrary",)),
        cost_estimate=pl.CostEstimate(
            flops=3_000_000_000, bytes_accessed=8_000_000, transcendentals=0
        ),
    )(band_rows, tokens, *sides, *params)


def body(
    tokens, band_rows, down_gain, down_shift, down_weight, up_weight, up_gain, up_shift, mix_weight
):
    members, levels, slots, columns, features = tokens.shape
    units = members * levels
    flat = tokens.reshape(units, slots, columns, features)
    live = band_rows[0, 1] - band_rows[0, 0]
    west = shifted(flat[:, :, columns - 1], "lon", 1)
    east = shifted(flat[:, :, 0], "lon", -1)

    def with_sides(row):
        pick = lambda array: lax.dynamic_slice_in_dim(array, row, 1, 1)
        return jnp.concatenate([pick(flat)[:, 0], pick(east), pick(west)], axis=1)

    north = passed_along(with_sides(live - 1), "lat", 1)
    south = passed_along(with_sides(0), "lat", -1)
    down = lax.all_gather(down_weight, ("lon", "lat"), axis=0, tiled=True)
    up = lax.all_gather(up_weight, ("lon", "lat"), axis=0, tiled=True)
    out = compute(
        flat, band_rows, (west, east, north, south),
        (down_gain, down_shift, up_gain, up_shift), (down, up, mix_weight),
    )
    return out.reshape(tokens.shape)


def solution(mesh):
    return jax.shard_map(
        body,
        mesh=mesh,
        in_specs=(
            P("mem", None, "lat", "lon", None),
            P("lat", None),
            P(),
            P(),
            P(("lon", "lat"), None),
            P(("lon", "lat"), None),
            P(),
            P(),
            P(),
        ),
        out_specs=P("mem", None, "lat", "lon", None),
        check_vma=False,
    )
```

```python
import functools

import jax
import jax.numpy as jnp
from jax import lax
from jax.experimental import pallas as pl
from jax.experimental.pallas import tpu as pltpu
from jax.sharding import PartitionSpec as P

MESH = pl.DeviceIdType.MESH


def normalized(planes, gains, shifts, width):
    total = functools.reduce(jnp.add, planes)
    average = jnp.sum(total, axis=-1, keepdims=True) * (1.0 / width)
    centred = [plane - average for plane in planes]
    squares = functools.reduce(jnp.add, [c * c for c in centred])
    spread = jnp.sum(squares, axis=-1, keepdims=True) * (1.0 / width)
    scale = lax.rsqrt(spread + 1e-05)
    return [
        (c * scale * gain + shift).astype(jnp.bfloat16)
        for c, gain, shift in zip(centred, gains, shifts)
    ]


def kernel(
    sizes, band_ref, tokens_ref, shards_ref, down_gain_ref, down_shift_ref,
    up_gain_ref, up_shift_ref, mix_ref, out_ref,
    held, west, east, north, south, last, gathered, down_wide, up_wide, down_all, up_all,
    merged, results,
    local_sem, send_lon, recv_lon, send_plane, recv_plane, send_twin, recv_twin,
    send_side, recv_side,
):
    n_lon, n_lat, n_mem = sizes
    members, slots, columns, levels, features = held.shape
    kinds, _, _, shard_rows, shard_cols = gathered.shape
    half_rows = slots // 2 + 1
    half_cols = columns // 2 + 1
    lon, lat, mem = lax.axis_index("lon"), lax.axis_index("lat"), lax.axis_index("mem")
    twin = lat + 1 - 2 * lax.rem(lat, 2)
    first_row = band_ref[0, 0]
    live = band_ref[0, 1] - first_row
    odd = lax.rem(first_row, 2)

    def wrap(value, size):
        return lax.rem(value + size, size)

    def at(d_lon=0, d_lat=0, d_mem=0):
        return (wrap(lon + d_lon, n_lon), wrap(lat + d_lat, n_lat), wrap(mem + d_mem, n_mem))

    peers = [(dx, dm) for dx in range(n_lat // 2) for dm in range(n_mem) if (dx, dm) != (0, 0)]
    around = [(a, b) for a in (-1, 0, 1) for b in (-1, 0, 1) if (a, b) != (0, 0)]

    own_tokens = pltpu.make_async_copy(tokens_ref, held, local_sem.at[0])
    own_tokens.start()
    own_shard = pltpu.make_async_copy(
        shards_ref.at[mem], gathered.at[mem, lon, lat], local_sem.at[1]
    )
    own_shard.start()

    barrier = pltpu.get_barrier_semaphore()
    others = [at(d) for d in range(1, n_lon)]
    others += [at(0, 2 * dx, dm) for dx, dm in peers]
    others += [(lon, twin, mem)]
    others += [at(a, b) for a, b in around]
    for other in others:
        pl.semaphore_signal(barrier, inc=1, device_id=other, device_id_type=MESH)

    own_tokens.wait()
    last[...] = held[:, jnp.clip(live - 1, 0, slots - 1)]
    own_shard.wait()
    pl.semaphore_wait(barrier, len(others))

    started = []

    def send(source, target, send_sem, recv_sem, device):
        copy = pltpu.make_async_remote_copy(
            src_ref=source, dst_ref=target, send_sem=send_sem, recv_sem=recv_sem,
            device_id=device, device_id_type=MESH,
        )
        copy.start()
        started.append(copy)

    def arrived(target, send_sem, recv_sem, device):
        pltpu.make_async_remote_copy(
            src_ref=target, dst_ref=target, send_sem=send_sem, recv_sem=recv_sem,
            device_id=device, device_id_type=MESH,
        ).wait_recv()

    mine = gathered.at[mem, lon, lat]
    for d in range(1, n_lon):
        send(mine, mine, send_lon.at[d], recv_lon.at[d], at(d))

    sides = []
    for index, (a, b) in enumerate(around):
        column = {-1: 0, 1: columns - 1}.get(a)
        slot = {-1: columns + 1, 1: 0}.get(a)
        if b == 0:
            source, target = held.at[:, :, column], (east if a < 0 else west)
        else:
            row = last if b > 0 else held.at[:, 0]
            place = north if b > 0 else south
            if a == 0:
                source, target = row, place.at[:, pl.ds(1, columns)]
                if b < 0:
                    source = held.at[:, 0]
            else:
                source = last.at[:, column] if b > 0 else held.at[:, 0, column]
                target = place.at[:, slot]
        send(source, target, send_side.at[index], recv_side.at[index], at(a, b))
        sides.append((target, index, at(-a, -b)))

    def to_plane(d):
        chunk = gathered.at[mem, wrap(lon - d, n_lon), lat]
        for k, (dx, dm) in enumerate(peers):
            send(chunk, chunk, send_plane.at[k, d], recv_plane.at[k, d], at(0, 2 * dx, dm))
        send(chunk, chunk, send_twin.at[0, d], recv_twin.at[0, d], (lon, twin, mem))

    to_plane(0)
    for d in range(1, n_lon):
        chunk = gathered.at[mem, wrap(lon - d, n_lon), lat]
        arrived(chunk, send_lon.at[d], recv_lon.at[d], at(-d))
        to_plane(d)

    for target, index, device in sides:
        arrived(target, send_side.at[index], recv_side.at[index], device)

    bottom = lat == n_lat - 1
    chunk_rows = max(r for r in range(1, 10) if half_rows % r == 0)
    chunks = half_rows // chunk_rows
    rows_each = chunk_rows * half_cols * levels
    gains = [down_gain_ref[i : i + 1] for i in range(4)]
    shifts = [down_shift_ref[i : i + 1] for i in range(4)]
    order = [(p, q) for q in range(2) for p in range(2)]

    def merge(step, carry):
        member, begin = step // chunks, lax.rem(step, chunks) * chunk_rows
        planes = {pq: [] for pq in order}
        for k in range(chunk_rows):
            for p in range(2):
                row = 2 * (begin + k) + p - odd
                safe = jnp.clip(row, 0, slots - 1)
                for c in range(columns + 2):
                    if c == 0:
                        cell = west[member, safe]
                    elif c == columns + 1:
                        cell = east[member, safe]
                    else:
                        cell = held[member, safe, c - 1]
                    cell = cell.astype(jnp.float32)
                    below = south[member, c].astype(jnp.float32)
                    below = jnp.where(bottom, jnp.zeros_like(below), below)
                    cell = jnp.where(row == live, below, cell)
                    if k == 0 and p == 0:
                        cell = jnp.where(row < 0, north[member, c].astype(jnp.float32), cell)
                    planes[p, c % 2].append(cell)
        parts = normalized(
            [jnp.concatenate(planes[pq], 0) for pq in order], gains, shifts, 4 * features
        )
        for i, part in enumerate(parts):
            merged[i, step] = part
        return carry

    lax.fori_loop(0, members * chunks, merge, 0)

    for d in range(n_lon):
        for k, (dx, dm) in enumerate(peers):
            chunk = gathered.at[
                wrap(mem - dm, n_mem), wrap(lon - d, n_lon), wrap(lat - 2 * dx, n_lat)
            ]
            arrived(chunk, send_plane.at[k, d], recv_plane.at[k, d], at(0, -2 * dx, -dm))
            send(
                chunk, chunk, send_twin.at[k + 1, d], recv_twin.at[k + 1, d], (lon, twin, mem)
            )
    for d in range(n_lon):
        for k, (dx, dm) in enumerate([(0, 0)] + peers):
            chunk = gathered.at[
                wrap(mem - dm, n_mem), wrap(lon - d, n_lon), wrap(twin - 2 * dx, n_lat)
            ]
            arrived(chunk, send_twin.at[k, d], recv_twin.at[k, d], (lon, twin, mem))

    half = shard_rows // 2
    for l in range(n_lon):
        for t in range(n_lat):
            place = l * n_lat + t
            down_wide[pl.ds(place * shard_rows, shard_rows), :] = gathered[0, l, t].astype(
                jnp.float32
            )
            block = gathered[1, l, t].astype(jnp.float32)
            for p in range(2):
                piece = block[p * half : (p + 1) * half]
                for q in range(2):
                    up_wide[2 * p + q, pl.ds(place * half, half), :] = piece[
                        :, q * features : (q + 1) * features
                    ]
    down_all[...] = down_wide[...].astype(jnp.bfloat16)
    for i in range(4):
        up_all[i] = up_wide[i].astype(jnp.bfloat16)

    def expand(step, carry):
        member, begin = step // chunks, lax.rem(step, chunks) * chunk_rows
        coarse = functools.reduce(
            jnp.add,
            [
                jnp.dot(
                    merged[i, step], down_all[i * features : (i + 1) * features],
                    preferred_element_type=jnp.float32,
                )
                for i in range(4)
            ],
        ).astype(jnp.bfloat16)
        for p in range(2):
            for q in range(2):
                grown = jnp.dot(coarse, up_all[2 * p + q], preferred_element_type=jnp.float32)
                (fine,) = normalized([grown], [up_gain_ref[...]], [up_shift_ref[...]], features)
                fine = jnp.dot(fine, mix_ref[...], preferred_element_type=jnp.float32)
                fine = fine.reshape(chunk_rows, half_cols, levels, features)
                for k in range(chunk_rows):
                    for j in range(half_cols):
                        column = 2 * j + q - 1
                        if 0 <= column < columns:
                            results[member, 2 * (begin + k) + p, column] = fine[k, j]
        return carry

    lax.fori_loop(0, members * chunks, expand, 0)

    def finish(row, carry):
        for member in range(members):
            values = results[member, row + odd]
            values = jnp.where(row < live, values, jnp.zeros_like(values))
            out_ref[member, row] = values.astype(jnp.bfloat16)
        return carry

    lax.fori_loop(0, slots, finish, 0)
    for copy in started:
        copy.wait_send()


def body(
    sizes, tokens, band_rows, down_gain, down_shift, down_weight, up_weight, up_gain, up_shift,
    mix_weight,
):
    n_lon, n_lat, n_mem = sizes
    members, levels, slots, columns, features = tokens.shape
    cells = tokens.transpose(0, 2, 3, 1, 4)
    up_rows, up_cols = up_weight.shape
    shard_rows, shard_cols = down_weight.shape
    up_folded = up_weight.reshape(up_rows, 2, up_cols // 2).transpose(1, 0, 2)
    shards = jnp.stack([down_weight, up_folded.reshape(shard_rows, shard_cols)])
    half_rows, half_cols = slots // 2 + 1, columns // 2 + 1
    chunk_rows = max(r for r in range(1, 10) if half_rows % r == 0)
    steps = members * half_rows // chunk_rows
    n_peers = n_lat // 2 * n_mem - 1
    n_all = n_lon * n_lat
    bf16, f32 = jnp.bfloat16, jnp.float32
    vmem = pl.BlockSpec(memory_space=pltpu.VMEM)
    dma = pltpu.SemaphoreType.DMA
    out = pl.pallas_call(
        functools.partial(kernel, sizes),
        out_shape=jax.ShapeDtypeStruct(cells.shape, cells.dtype),
        in_specs=[
            pl.BlockSpec(memory_space=pltpu.SMEM), pl.BlockSpec(memory_space=pl.ANY),
            vmem, vmem, vmem, vmem, vmem, vmem,
        ],
        out_specs=vmem,
        scratch_shapes=[
            pltpu.VMEM(cells.shape, bf16),
            pltpu.VMEM((members, slots, levels, features), bf16),
            pltpu.VMEM((members, slots, levels, features), bf16),
            pltpu.VMEM((members, columns + 2, levels, features), bf16),
            pltpu.VMEM((members, columns + 2, levels, features), bf16),
            pltpu.VMEM((members, columns, levels, features), bf16),
            pltpu.VMEM((2, n_lon, n_lat, shard_rows, shard_cols), bf16),
            pltpu.VMEM((n_all * shard_rows, shard_cols), f32),
            pltpu.VMEM((4, n_all * up_rows, features), f32),
            pltpu.VMEM((n_all * shard_rows, shard_cols), bf16),
            pltpu.VMEM((4, n_all * up_rows, features), bf16),
            pltpu.VMEM((4, steps, chunk_rows * half_cols * levels, features), bf16),
            pltpu.VMEM((members, 2 * half_rows, columns, levels, features), f32),
            dma((2,)),
            dma((n_lon,)), dma((n_lon,)),
            dma((n_peers, n_lon)), dma((n_peers, n_lon)),
            dma((n_peers + 1, n_lon)), dma((n_peers + 1, n_lon)),
            dma((8,)), dma((8,)),
        ],
        compiler_params=pltpu.CompilerParams(collective_id=0, has_side_effects=True),
        cost_estimate=pl.CostEstimate(
            flops=3_000_000_000, bytes_accessed=8_000_000, transcendentals=0
        ),
    )(
        band_rows, cells, shards, down_gain.reshape(4, features), down_shift.reshape(4, features),
        up_gain.reshape(1, features), up_shift.reshape(1, features), mix_weight,
    )
    return out.transpose(0, 3, 1, 2, 4)


def solution(mesh):
    sizes = tuple(mesh.shape[name] for name in ("lon", "lat", "mem"))
    assert sizes[2] == 2
    return jax.shard_map(
        functools.partial(body, sizes),
        mesh=mesh,
        in_specs=(
            P("mem", None, "lat", "lon", None),
            P("lat", None),
            P(),
            P(),
            P(("lon", "lat"), None),
            P(("lon", "lat"), None),
            P(),
            P(),
            P(),
        ),
        out_specs=P("mem", None, "lat", "lon", None),
        check_vma=False,
    )
```

```python
import functools
import math

import jax
import jax.numpy as jnp
from jax import lax
from jax.experimental import pallas as pl
from jax.experimental.pallas import tpu as pltpu
from jax.sharding import PartitionSpec as P

MESH = pl.DeviceIdType.MESH


def normalized(planes, gains, shifts, width):
    total = functools.reduce(jnp.add, planes)
    average = jnp.sum(total, axis=-1, keepdims=True) * (1.0 / width)
    centred = [plane - average for plane in planes]
    squares = functools.reduce(jnp.add, [c * c for c in centred])
    spread = jnp.sum(squares, axis=-1, keepdims=True) * (1.0 / width)
    scale = lax.rsqrt(spread + 1e-05)
    return [
        (c * scale * gain + shift).astype(jnp.bfloat16)
        for c, gain, shift in zip(centred, gains, shifts)
    ]


def kernel(
    sizes, band_ref, tokens_ref, down_ref, up_ref, down_gain_ref, down_shift_ref,
    up_gain_ref, up_shift_ref, mix_ref, out_ref,
    held, west, east, to_west, to_east, north, south, last, gathered, down_wide, up_wide, down_all, up_all,
    merged, results,
    local_sem, send_lon, recv_lon, send_plane, recv_plane, send_twin, recv_twin,
    send_side, recv_side,
):
    n_lon, n_lat, n_mem = sizes
    members, slots, columns, levels, features = held.shape
    _, _, _, shard_blocks, block_rows, shard_cols = gathered.shape
    shard_rows = shard_blocks * block_rows
    half_rows = slots // 2 + 1
    half_cols = columns // 2 + 1
    lon, lat, mem = lax.axis_index("lon"), lax.axis_index("lat"), lax.axis_index("mem")
    twin = lat + 1 - 2 * lax.rem(lat, 2)
    first_row = band_ref[0, 0]
    live = band_ref[0, 1] - first_row
    odd = lax.rem(first_row, 2)

    def wrap(value, size):
        return lax.rem(value + size, size)

    def at(d_lon=0, d_lat=0, d_mem=0):
        return (wrap(lon + d_lon, n_lon), wrap(lat + d_lat, n_lat), wrap(mem + d_mem, n_mem))

    peers = [(dx, dm) for dx in range(n_lat // 2) for dm in range(n_mem) if (dx, dm) != (0, 0)]
    around = [(0, 1), (0, -1), (1, 1), (1, -1), (-1, 1), (-1, -1), (1, 0), (-1, 0)]

    own_tokens = pltpu.make_async_copy(tokens_ref, held, local_sem.at[0])
    own_tokens.start()
    half_blocks = shard_blocks // 2
    down_copy = pltpu.make_async_copy(down_ref, gathered.at[0, lon, lat], local_sem.at[1])
    up_copies = [
        pltpu.make_async_copy(
            up_ref.at[:, :, pl.ds(p * shard_cols, shard_cols)],
            gathered.at[1, lon, lat, pl.ds(p * half_blocks, half_blocks)],
            local_sem.at[2 + p],
        )
        for p in range(2)
    ]

    @pl.when(mem == 0)
    def _():
        down_copy.start()

    @pl.when(mem == 1)
    def _():
        for copy in up_copies:
            copy.start()

    barrier = pltpu.get_barrier_semaphore()
    others = [at(d) for d in range(1, n_lon)]
    others += [at(0, 2 * dx, dm) for dx, dm in peers]
    others += [(lon, twin, mem)]
    others += [at(a, b) for a, b in around]
    for other in others:
        pl.semaphore_signal(barrier, inc=1, device_id=other, device_id_type=MESH)

    own_tokens.wait()
    for packed, column in ((to_west, 0), (to_east, columns - 1)):
        packed[...] = jnp.concatenate(
            [held[m, :, column].astype(jnp.float32) for m in range(members)], -1
        ).astype(jnp.bfloat16)
    last[...] = held[:, jnp.clip(live - 1, 0, slots - 1)]

    @pl.when(mem == 0)
    def _():
        down_copy.wait()

    @pl.when(mem == 1)
    def _():
        for copy in up_copies:
            copy.wait()

    pl.semaphore_wait(barrier, len(others))

    started = []

    def send(source, target, send_sem, recv_sem, device):
        copy = pltpu.make_async_remote_copy(
            src_ref=source, dst_ref=target, send_sem=send_sem, recv_sem=recv_sem,
            device_id=device, device_id_type=MESH,
        )
        copy.start()
        started.append(copy)

    def arrived(target, send_sem, recv_sem, device):
        pltpu.make_async_remote_copy(
            src_ref=target, dst_ref=target, send_sem=send_sem, recv_sem=recv_sem,
            device_id=device, device_id_type=MESH,
        ).wait_recv()

    mine = gathered.at[mem, lon, lat]
    for d in range(1, n_lon):
        send(mine, mine, send_lon.at[d], recv_lon.at[d], at(d))

    sides = []
    for index, (a, b) in enumerate(around):
        column = {-1: 0, 1: columns - 1}.get(a)
        slot = {-1: columns + 1, 1: 0}.get(a)
        if b == 0:
            source, target = (to_west, east) if a < 0 else (to_east, west)
        else:
            row = last if b > 0 else held.at[:, 0]
            place = north if b > 0 else south
            if a == 0:
                source, target = row, place.at[:, pl.ds(1, columns)]
                if b < 0:
                    source = held.at[:, 0]
            else:
                source = last.at[:, column] if b > 0 else held.at[:, 0, column]
                target = place.at[:, slot]
        send(source, target, send_side.at[index], recv_side.at[index], at(a, b))
        sides.append((target, index, at(-a, -b)))

    def to_plane(d):
        chunk = gathered.at[mem, wrap(lon - d, n_lon), lat]
        for k, (dx, dm) in enumerate(peers):
            send(chunk, chunk, send_plane.at[k, d], recv_plane.at[k, d], at(0, 2 * dx, dm))
        send(chunk, chunk, send_twin.at[0, d], recv_twin.at[0, d], (lon, twin, mem))

    to_plane(0)
    for d in range(1, n_lon):
        chunk = gathered.at[mem, wrap(lon - d, n_lon), lat]
        arrived(chunk, send_lon.at[d], recv_lon.at[d], at(-d))
        to_plane(d)

    bottom = lat == n_lat - 1
    chunk_rows = max(r for r in range(1, 10) if half_rows % r == 0)
    chunks = half_rows // chunk_rows
    gain_row = down_gain_ref[...].reshape(1, 4 * features)
    shift_row = down_shift_ref[...].reshape(1, 4 * features)
    gains = [gain_row[:, i * features : (i + 1) * features] for i in range(4)]
    shifts = [shift_row[:, i * features : (i + 1) * features] for i in range(4)]
    order = [(p, q) for q in range(2) for p in range(2)]

    def merge(pairs, rows_done, step, carry):
        begin = step * chunk_rows
        planes = {pq: [] for pq in order}
        for member in range(members):
            lanes = slice(member * features, (member + 1) * features)
            for k in range(chunk_rows):
                for p in range(2):
                    row = 2 * (begin + k) + p - odd
                    safe = jnp.clip(row, 0, slots - 1)
                    for c in [2 * j + q for j in pairs for q in range(2)]:
                        if c == 0:
                            cell = west[safe][:, lanes]
                        elif c == columns + 1:
                            cell = east[safe][:, lanes]
                        else:
                            cell = held[member, safe, c - 1]
                        cell = cell.astype(jnp.float32)
                        below = south[member, c].astype(jnp.float32)
                        below = jnp.where(bottom, jnp.zeros_like(below), below)
                        cell = jnp.where(row == live, below, cell)
                        if k == 0 and p == 0:
                            cell = jnp.where(row < 0, north[member, c].astype(jnp.float32), cell)
                        planes[p, c % 2].append(cell)
        parts = normalized(
            [jnp.concatenate(planes[pq], 0) for pq in order], gains, shifts, 4 * features
        )
        for i, part in enumerate(parts):
            merged[i, rows_done + step, : part.shape[0]] = part
        return carry

    def expand(pairs, rows_done, step, carry):
        begin = step * chunk_rows
        cells = members * chunk_rows * len(pairs)
        coarse = functools.reduce(
            jnp.add,
            [
                jnp.dot(
                    merged[i, rows_done + step, : cells * levels],
                    down_all[i * features : (i + 1) * features],
                    preferred_element_type=jnp.float32,
                )
                for i in range(4)
            ],
        ).astype(jnp.bfloat16)
        for p in range(2):
            for q in range(2):
                grown = jnp.dot(coarse, up_all[2 * p + q], preferred_element_type=jnp.float32)
                (fine,) = normalized([grown], [up_gain_ref[...]], [up_shift_ref[...]], features)
                fine = jnp.dot(fine, mix_ref[...], preferred_element_type=jnp.float32)
                fine = fine.reshape(members, chunk_rows, len(pairs), levels, features)
                for member in range(members):
                    for k in range(chunk_rows):
                        for at_pair, j in enumerate(pairs):
                            column = 2 * j + q - 1
                            if 0 <= column < columns:
                                results[member, 2 * (begin + k) + p, column] = fine[
                                    member, k, at_pair
                                ].astype(jnp.bfloat16)
        return carry

    inner, edges = tuple(range(1, half_cols - 1)), (0, half_cols - 1)

    def settle(which):
        for (a, b), (target, index, device) in zip(around, sides):
            if (a == 0) == which:
                arrived(target, send_side.at[index], recv_side.at[index], device)

    settle(True)
    lax.fori_loop(0, chunks, functools.partial(merge, inner, 0), 0)

    for d in range(n_lon):
        for k, (dx, dm) in enumerate(peers):
            chunk = gathered.at[
                wrap(mem - dm, n_mem), wrap(lon - d, n_lon), wrap(lat - 2 * dx, n_lat)
            ]
            arrived(chunk, send_plane.at[k, d], recv_plane.at[k, d], at(0, -2 * dx, -dm))
            send(
                chunk, chunk, send_twin.at[k + 1, d], recv_twin.at[k + 1, d], (lon, twin, mem)
            )
    for d in range(n_lon):
        for k, (dx, dm) in enumerate([(0, 0)] + peers):
            chunk = gathered.at[
                wrap(mem - dm, n_mem), wrap(lon - d, n_lon), wrap(twin - 2 * dx, n_lat)
            ]
            arrived(chunk, send_twin.at[k, d], recv_twin.at[k, d], (lon, twin, mem))

    half = shard_rows // 2
    for l in range(n_lon):
        for t in range(n_lat):
            place = l * n_lat + t
            down_wide[pl.ds(place * shard_rows, shard_rows), :] = gathered[0, l, t].astype(
                jnp.float32
            ).reshape(shard_rows, shard_cols)
            block = gathered[1, l, t].astype(jnp.float32).reshape(shard_rows, shard_cols)
            for p in range(2):
                piece = block[p * half : (p + 1) * half]
                for q in range(2):
                    up_wide[2 * p + q, pl.ds(place * half, half), :] = piece[
                        :, q * features : (q + 1) * features
                    ]
    down_all[...] = down_wide[...].astype(jnp.bfloat16)
    for i in range(4):
        up_all[i] = up_wide[i].astype(jnp.bfloat16)

    lax.fori_loop(0, chunks, functools.partial(expand, inner, 0), 0)
    settle(False)
    lax.fori_loop(0, chunks, functools.partial(merge, edges, chunks), 0)
    lax.fori_loop(0, chunks, functools.partial(expand, edges, chunks), 0)

    def finish(row, carry):
        for member in range(members):
            values = results[member, row + odd]
            values = jnp.where(row < live, values, jnp.zeros_like(values))
            out_ref[member, row] = values
        return carry

    lax.fori_loop(0, slots, finish, 0)
    for copy in started:
        copy.wait_send()


def body(
    sizes, tokens, band_rows, down_gain, down_shift, down_weight, up_weight, up_gain, up_shift,
    mix_weight,
):
    n_lon, n_lat, n_mem = sizes
    members, levels, slots, columns, features = tokens.shape
    cells = tokens.transpose(0, 2, 3, 1, 4)
    up_rows, up_cols = up_weight.shape
    shard_rows, shard_cols = down_weight.shape
    block_rows = math.gcd(up_rows, 8)
    half_rows, half_cols = slots // 2 + 1, columns // 2 + 1
    chunk_rows = max(r for r in range(1, 10) if half_rows % r == 0)
    steps = 2 * half_rows // chunk_rows
    widest = members * chunk_rows * max(2, half_cols - 2) * levels
    n_peers = n_lat // 2 * n_mem - 1
    n_all = n_lon * n_lat
    bf16, f32 = jnp.bfloat16, jnp.float32
    vmem = pl.BlockSpec(memory_space=pltpu.VMEM)
    dma = pltpu.SemaphoreType.DMA
    out = pl.pallas_call(
        functools.partial(kernel, sizes),
        out_shape=pltpu.VMEM(cells.shape, cells.dtype),
        in_specs=[
            pl.BlockSpec(memory_space=pltpu.SMEM), pl.BlockSpec(memory_space=pl.ANY),
            vmem, vmem, vmem, vmem, vmem, vmem, vmem,
        ],
        out_specs=vmem,
        scratch_shapes=[
            pltpu.VMEM(cells.shape, bf16),
            pltpu.VMEM((slots, levels, members * features), bf16),
            pltpu.VMEM((slots, levels, members * features), bf16),
            pltpu.VMEM((slots, levels, members * features), bf16),
            pltpu.VMEM((slots, levels, members * features), bf16),
            pltpu.VMEM((members, columns + 2, levels, features), bf16),
            pltpu.VMEM((members, columns + 2, levels, features), bf16),
            pltpu.VMEM((members, columns, levels, features), bf16),
            pltpu.VMEM((2, n_lon, n_lat, shard_rows // block_rows, block_rows, shard_cols), bf16),
            pltpu.VMEM((n_all * shard_rows, shard_cols), f32),
            pltpu.VMEM((4, n_all * up_rows, features), f32),
            pltpu.VMEM((n_all * shard_rows, shard_cols), bf16),
            pltpu.VMEM((4, n_all * up_rows, features), bf16),
            pltpu.VMEM((4, steps, widest, features), bf16),
            pltpu.VMEM((members, 2 * half_rows, columns, levels, features), bf16),
            dma((4,)),
            dma((n_lon,)), dma((n_lon,)),
            dma((n_peers, n_lon)), dma((n_peers, n_lon)),
            dma((n_peers + 1, n_lon)), dma((n_peers + 1, n_lon)),
            dma((8,)), dma((8,)),
        ],
        compiler_params=pltpu.CompilerParams(collective_id=0, has_side_effects=True),
        cost_estimate=pl.CostEstimate(
            flops=3_000_000_000, bytes_accessed=8_000_000, transcendentals=0
        ),
    )(
        band_rows, cells, down_weight.reshape(-1, block_rows, shard_cols),
        up_weight.reshape(-1, block_rows, up_cols), down_gain, down_shift,
        up_gain.reshape(1, features), up_shift.reshape(1, features), mix_weight,
    )
    return out.transpose(0, 3, 1, 2, 4)


def solution(mesh):
    sizes = tuple(mesh.shape[name] for name in ("lon", "lat", "mem"))
    assert sizes[2] == 2
    return jax.shard_map(
        functools.partial(body, sizes),
        mesh=mesh,
        in_specs=(
            P("mem", None, "lat", "lon", None),
            P("lat", None),
            P(),
            P(),
            P(("lon", "lat"), None),
            P(("lon", "lat"), None),
            P(),
            P(),
            P(),
        ),
        out_specs=P("mem", None, "lat", "lon", None),
        check_vma=False,
    )
```
